32 devices in a mesh: rows: 32 (over z, y, x, core).
Axes of the slice: x: 2, y: 2, z: 4, core: 2. Of those that a mesh axis runs over, the one named last changes fastest.
Arguments:
- left_factor: float32 [65536, 1024], P('rows'), may hold values from -6 to 6
- right_factor: float32 [65536, 1024], P('rows'), may hold values from -6 to 6
- tile_counts: int32 [32], P('rows'), may hold values from 1 to 4, as said below
- start_basis: float32 [1024, 256], replicated, may hold values from -6 to 6
Outputs:
- left_proj: float32 [65536, 256], P('rows')
- right_proj: float32 [65536, 256], P('rows')
The draws below stay inside these ranges and needn't reach their ends.
Inputs may be any that keep to these rules, and one draw needn't show every extreme that they name: `tile_counts`: each device's live slots are its first ones; some device has 4 live slots and some device has 1.
All inputs are finite; a program needn't handle non-finite values.
Results may differ from the reference program's by a relative error of at most 0.0002.
Values sent between devices are 32-bit elements; how exact they have to be, the bound alone decides.
No kernel may reach another device: no remote copies, remote signals or barrier semaphores. Data moves between devices by JAX's collectives and lax.ppermute only.
A program may use at most 128 MiB of HBM per device.

```python
import jax
import jax.numpy as jnp
from jax import lax

STATES = 1024
RANK = 256
TILE = 512
SLOTS = 4
POWER = 2
ROWS_ALL = 65536
N_ROWS = 32


def draw_tile_counts(key, part):
    kinds = jax.random.randint(jax.random.fold_in(key, 11), (N_ROWS,), 0, 4)
    middle = max(1, SLOTS // 2)
    counts = jnp.where(kinds < 2, 1, jnp.where(kinds == 2, middle, SLOTS)).astype(jnp.int32)
    heavy = jax.random.randint(jax.random.fold_in(key, 12), (), 0, N_ROWS)
    offset = jax.random.randint(jax.random.fold_in(key, 13), (), 1, N_ROWS)
    light = (heavy + offset) % N_ROWS
    positions = jnp.arange(N_ROWS, dtype=jnp.int32)
    counts = jnp.where(positions == heavy, SLOTS, counts)
    counts = jnp.where(positions == light, 1, counts)
    return counts.astype(jnp.int32)


def steps_of(rng, shape, pieces, least, high):
    loudness = 1.0
    for position, blocks in pieces:
        heights = jax.random.uniform(jax.random.fold_in(jax.random.fold_in(rng, 6), position), (blocks,), jnp.float32, least / len(pieces), high / len(pieces))
        loudness = loudness * jnp.repeat(jnp.exp(heights), shape[position] // blocks).reshape((-1,) + (1,) * (len(shape) - 1 - position))
    return loudness


def normal_values(key, extent, scale, reach, cuts=(), kind=jnp.bfloat16):
    result = scale * jax.random.normal(key, extent, jnp.float32)
    if cuts:
        result = result * steps_of(key, extent, cuts, -0.22, 0.18)
    return jnp.clip(result, -reach, reach).astype(kind)


def setup_inputs(seed: int = 0) -> dict:
    seeds = jax.random.split(jax.random.key(seed), 5)
    return {
        "left_factor": normal_values(seeds[0], (ROWS_ALL, STATES), 1.0, 6.0, ((0, 32),), jnp.float32),
        "right_factor": normal_values(seeds[1], (ROWS_ALL, STATES), 1.0, 6.0, ((0, 32),), jnp.float32),
        "tile_counts": draw_tile_counts(jax.random.fold_in(seeds[4], 71), 0),
        "start_basis": normal_values(seeds[3], (STATES, RANK), 1.0, 6.0, (), jnp.float32),
    }


def product(left_side, right_side):
    return jnp.dot(left_side.astype(jnp.float32), right_side.astype(jnp.float32), precision=lax.Precision.HIGHEST, preferred_element_type=jnp.float32)

def transposed_product(left_side, right_side):
    return lax.dot_general(left_side.astype(jnp.float32), right_side.astype(jnp.float32), (((0,), (0,)), ((), ())), precision=lax.Precision.HIGHEST, preferred_element_type=jnp.float32)

def right_solve(factor, block):
    return jax.scipy.linalg.solve_triangular(factor, block.T, lower=True).T

def orthonormal(block):
    factor = jnp.linalg.cholesky(transposed_product(block, block))
    return right_solve(factor, block)

def reference(left_factor, right_factor, tile_counts, start_basis):
    devices = tile_counts.shape[0]
    slot_ids = jnp.arange(SLOTS, dtype=jnp.int32)
    live_slots = (slot_ids[None, :] < tile_counts[:, None]).astype(left_factor.dtype)
    row_mask = jnp.broadcast_to(live_slots[:, :, None], (devices, SLOTS, TILE)).reshape(-1, 1)
    gram_matrix = transposed_product(left_factor, right_factor * row_mask)
    current = start_basis
    for iteration in range(POWER):
        current = orthonormal(transposed_product(gram_matrix, product(gram_matrix, current)))
    image_cols = product(gram_matrix, current)
    square = transposed_product(image_cols, image_cols)
    factor = jnp.linalg.cholesky(square)
    left_map = right_solve(factor, image_cols)
    scaling = jnp.sqrt(jnp.trace(square) / RANK)
    right_map = right_solve(factor, current) * scaling
    left_proj = product(left_factor, left_map) * row_mask
    right_proj = product(right_factor, right_map) * row_mask
    return (left_proj, right_proj)
```

```python
import functools

import jax
import jax.numpy as jnp
from jax import lax
from jax.experimental import pallas as pl
from jax.experimental.pallas import tpu as pltpu
from jax.sharding import PartitionSpec as P

SLOTS = 4
POWER = 2
STEP = 16
LANES = 128

ROWS_BY_ROWS = (((1,), (1,)), ((), ()))
ROWS_BY_COLS = (((1,), (0,)), ((), ()))
COLS_BY_COLS = (((0,), (0,)), ((), ()))


def mxu(a, b, dims):
    return lax.dot_general(a, b, dims, preferred_element_type=jnp.float32)


def two(x):
    high = x.astype(jnp.bfloat16)
    return high, (x - high.astype(jnp.float32)).astype(jnp.bfloat16)


def three(x):
    high = x.astype(jnp.bfloat16)
    rest = x - high.astype(jnp.float32)
    middle = rest.astype(jnp.bfloat16)
    return high, middle, (rest - middle.astype(jnp.float32)).astype(jnp.bfloat16)


def product(a, b, dims):
    return mxu(a[0], b[0], dims) + (mxu(a[0], b[1], dims) + mxu(a[1], b[0], dims))


def row_gram(x):
    high, middle, low = three(x)
    side = mxu(high, middle, ROWS_BY_ROWS) + mxu(high, low, ROWS_BY_ROWS)
    return (
        mxu(high, high, ROWS_BY_ROWS) + (side + side.T) + mxu(middle, middle, ROWS_BY_ROWS)
    )


def thin_product(left, right):
    a, b, c = three(left)
    d, e, f = three(right)
    return mxu(
        jnp.concatenate([a, a, b, b, a, c], axis=0),
        jnp.concatenate([d, e, d, e, f, d], axis=0),
        COLS_BY_COLS,
    )


def eliminate_slab(work, first, size):
    tiles = STEP // 8
    lane0 = first // LANES * LANES
    rows = pl.ds(first, STEP)
    left_end = size + min(size, (first + STEP + LANES - 1) // LANES * LANES)
    lanes = list(range(lane0, size, LANES)) + list(range(size, left_end, LANES))
    diag = work[rows, pl.ds(lane0, LANES)]
    panel = [[work[pl.ds(first + 8 * t, 8), pl.ds(l, LANES)] for l in lanes] for t in range(tiles)]
    column = [
        [
            jnp.broadcast_to(
                diag[8 * t : 8 * t + 8, first - lane0 + k : first - lane0 + k + 1], (8, LANES)
            )
            for t in range(tiles)
        ]
        for k in range(STEP)
    ]
    sublane = lax.broadcasted_iota(jnp.int32, (8, LANES), 0)
    pivots = [jnp.ones((8, LANES), jnp.float32) for t in range(tiles)]

    def spread(value, row):
        return jnp.broadcast_to(value[row : row + 1, :], (8, LANES))

    for j in range(STEP):
        t0, r = divmod(j, 8)
        pivot = spread(column[j][t0], r)
        pivots[t0] = jnp.where(sublane == r, pivot, pivots[t0])
        if j == STEP - 1:
            break
        inverse = 1.0 / pivot
        pivot_row = [spread(v, r) for v in panel[t0]]
        heads = {k: spread(column[k][t0], r) for k in range(j + 1, STEP)}
        for t in range(t0, tiles):
            if t == t0 and r == 7:
                continue
            factor = column[j][t] * inverse
            if t == t0:
                factor = jnp.where(sublane > r, factor, 0.0)
            panel[t] = [v - factor * p for v, p in zip(panel[t], pivot_row)]
            for k in range(j + 1, STEP):
                column[k][t] = column[k][t] - factor * heads[k]
    roots = [lax.rsqrt(p) for p in pivots]
    panel = [[v * roots[t] for v in panel[t]] for t in range(tiles)]
    slab = jnp.concatenate([jnp.concatenate(p, axis=1) for p in panel], axis=0)
    for i, l in enumerate(lanes):
        work[rows, pl.ds(l, LANES)] = slab[:, i * LANES : (i + 1) * LANES]
    below = first + STEP
    if below < size:
        start = below // LANES * LANES
        skip = start - lane0
        update = thin_product(slab[:, skip : size - lane0], slab[:, skip:])
        rest = pl.ds(below, size - below)
        for i, l in enumerate(lanes[skip // LANES :]):
            work[rest, pl.ds(l, LANES)] = (
                work[rest, pl.ds(l, LANES)] - update[below - start :, i * LANES : (i + 1) * LANES]
            )


def inverse_factor(work, square, size):
    row = lax.broadcasted_iota(jnp.int32, (size, size), 0)
    col = lax.broadcasted_iota(jnp.int32, (size, size), 1)
    work[:, :size] = square
    work[:, size:] = (row == col).astype(jnp.float32)
    for first in range(0, size, STEP):
        eliminate_slab(work, first, size)
    return work[:, size:]


def chain_kernel(
    place, kept_a, sent_a, kept_b, sent_b, start, out_lh, out_ll, out_rh, out_rl,
    high, low, current, image, work, scale
):
    half = kept_a.shape[0]
    mine = place[0]
    for part, (kept, sent) in enumerate(((kept_a, sent_a), (kept_b, sent_b))):
        for ref, side in ((kept, mine), (sent, 1 - mine)):
            at = pl.ds(pl.multiple_of((2 * part + side) * half, half), half)
            high[at, :], low[at, :] = two(ref[...])
    current[0] = start[...]
    rank = start.shape[0]

    def turn(step, carry):
        now = step % 2
        product_t = product(two(current[now]), (high[...], low[...]), ROWS_BY_ROWS)

        @pl.when(step < POWER)
        def _():
            image[...] = product(two(product_t), (high[...], low[...]), ROWS_BY_COLS)

        @pl.when(step == POWER)
        def _():
            image[...] = product_t
            scale[0] = jnp.sqrt(jnp.sum(product_t * product_t) / rank)

        inverse = inverse_factor(work, row_gram(image[...]), rank)
        current[1 - now] = product(two(inverse), two(image[...]), ROWS_BY_COLS)
        return carry

    lax.fori_loop(0, POWER + 1, turn, 0)
    out_lh[...], out_ll[...] = two(current[(POWER + 1) % 2])
    right = product(two(work[:, rank:]), two(current[POWER % 2]), ROWS_BY_COLS) * scale[0]
    out_rh[...], out_rl[...] = two(right)


def chain(place, kept_a, sent_a, kept_b, sent_b, start):
    rank, states = start.shape
    whole = pl.BlockSpec(memory_space=pltpu.VMEM)
    half = jax.ShapeDtypeStruct((rank, states), jnp.bfloat16)
    return pl.pallas_call(
        chain_kernel,
        out_shape=[half] * 4,
        in_specs=[pl.BlockSpec(memory_space=pltpu.SMEM)] + [whole] * 5,
        out_specs=[whole] * 4,
        scratch_shapes=[
            pltpu.VMEM((states, states), jnp.bfloat16),
            pltpu.VMEM((states, states), jnp.bfloat16),
            pltpu.VMEM((2, rank, states), jnp.float32),
            pltpu.VMEM((rank, states), jnp.float32),
            pltpu.VMEM((rank, 2 * rank), jnp.float32),
            pltpu.SMEM((1,), jnp.float32),
        ],
        compiler_params=pltpu.CompilerParams(vmem_limit_bytes=56 * 2**20),
        name="chain",
    )(place, kept_a, sent_a, kept_b, sent_b, start)


def gram_kernel(info, left_kept, left_sent, right, out_kept, out_sent):
    slot = pl.program_id(0)

    @pl.when(slot < info[0])
    def _():
        high, low = two(right[...])
        stack = jnp.concatenate([high, low, high], axis=0)
        for left, out in ((left_sent, out_sent), (left_kept, out_kept)):
            head, tail = two(left[...].T)
            term = mxu(jnp.concatenate([head, head, tail], axis=1), stack, ROWS_BY_COLS)

            @pl.when(slot == 0)
            def _():
                out[...] = term

            @pl.when(slot > 0)
            def _():
                out[...] += term


def gram_part(info, left, right, part, parts):
    rows, states = left.shape
    tile = rows // SLOTS
    half = states // parts // 2

    def at(slot, info):
        return jnp.minimum(slot, info[0] - 1)

    out = jax.ShapeDtypeStruct((half, states), jnp.float32)
    whole = pl.BlockSpec((half, states), lambda slot, info: (0, 0))
    return pl.pallas_call(
        gram_kernel,
        out_shape=[out, out],
        grid_spec=pltpu.PrefetchScalarGridSpec(
            num_scalar_prefetch=1,
            grid=(SLOTS,),
            in_specs=[
                pl.BlockSpec((tile, half), lambda slot, info: (at(slot, info), 2 * part + info[1])),
                pl.BlockSpec((tile, half), lambda slot, info: (at(slot, info), 2 * part + 1 - info[1])),
                pl.BlockSpec((tile, states), lambda slot, info: (at(slot, info), 0)),
            ],
            out_specs=[whole, whole],
        ),
        compiler_params=pltpu.CompilerParams(vmem_limit_bytes=56 * 2**20),
        cost_estimate=pl.CostEstimate(
            flops=12 * rows * half * states, bytes_accessed=4 * rows * states, transcendentals=0
        ),
        name=f"gram_{part}",
    )(info, left, left, right)


def project_kernel(info, left, right, map_lh, map_ll, map_rh, map_rl, out_left, out_right):
    slot = pl.program_id(0)
    live = slot < info[0]

    @pl.when(live)
    def _():
        out_left[...] = product(two(left[...]), (map_lh[...], map_ll[...]), ROWS_BY_ROWS)
        out_right[...] = product(two(right[...]), (map_rh[...], map_rl[...]), ROWS_BY_ROWS)

    @pl.when(jnp.logical_not(live))
    def _():
        out_left[...] = jnp.zeros_like(out_left)
        out_right[...] = jnp.zeros_like(out_right)


def project(info, left, right, maps):
    rows, states = left.shape
    rank = maps[0].shape[0]
    tile = rows // SLOTS

    def at(slot, info):
        return (jnp.minimum(slot, info[0] - 1), 0)

    out = jax.ShapeDtypeStruct((rows, rank), jnp.float32)
    return pl.pallas_call(
        project_kernel,
        out_shape=[out, out],
        grid_spec=pltpu.PrefetchScalarGridSpec(
            num_scalar_prefetch=1,
            grid=(SLOTS,),
            in_specs=[pl.BlockSpec((tile, states), at)] * 2
            + [pl.BlockSpec((rank, states), lambda slot, info: (0, 0))] * 4,
            out_specs=[pl.BlockSpec((tile, rank), lambda slot, info: (slot, 0))] * 2,
        ),
        compiler_params=pltpu.CompilerParams(vmem_limit_bytes=56 * 2**20),
        name="project",
    )(info, left, right, *maps)


class Pairs:
    def __init__(self, devices, bit):
        self.bit = bit
        self.table = [(i, i ^ (1 << bit)) for i in range(devices)]

    def side(self):
        return (lax.axis_index("rows") >> self.bit) & 1

    def swap(self, block):
        return lax.ppermute(block, "rows", self.table)

    def reduce_scatter(self, block):
        half = block.shape[0] // 2
        mine = self.side()
        away = self.swap(lax.dynamic_slice_in_dim(block, (1 - mine) * half, half, 0))
        return lax.dynamic_slice_in_dim(block, mine * half, half, 0) + away

    def all_gather(self, piece):
        away = self.swap(piece)
        second = self.side() == 1
        return jnp.concatenate(
            [jnp.where(second, away, piece), jnp.where(second, piece, away)], axis=0
        )


def make_local(devices):
    bits = devices.bit_length() - 1
    core = Pairs(devices, 0)
    others = [Pairs(devices, bit) for bit in range(1, bits)]
    orders = (others, others[1:] + others[:1])

    def local(left_factor, right_factor, tile_counts, start_basis):
        side = core.side()
        info = jnp.stack([tile_counts[0], side]).astype(jnp.int32)
        start = start_basis.T
        terms = [gram_part(info, left_factor, right_factor, part, len(orders)) for part in range(len(orders))]
        blocks = []
        for (kept, sent), order in zip(terms, orders):
            block = kept + core.swap(sent)
            for pairs in order:
                block = pairs.reduce_scatter(block)
            for pairs in reversed(order):
                block = pairs.all_gather(block)
            blocks += [block, core.swap(block)]
        maps = chain(info[1:], *blocks, start)
        return project(info, left_factor, right_factor, maps)

    return local


def solution(mesh):
    return jax.shard_map(
        make_local(mesh.shape["rows"]),
        mesh=mesh,
        in_specs=(P("rows", None), P("rows", None), P("rows"), P()),
        out_specs=(P("rows", None), P("rows", None)),
        check_vma=False,
    )
```

```python
import functools

import jax
import jax.numpy as jnp
from jax import lax
from jax.experimental import pallas as pl
from jax.experimental.pallas import tpu as pltpu
from jax.sharding import PartitionSpec as P

SLOTS = 4
POWER = 2
STEP = 16
COLUMNS = 256
PARTS = 2
PIECES = 1
LANES = 128

ROWS_BY_ROWS = (((1,), (1,)), ((), ()))
ROWS_BY_COLS = (((1,), (0,)), ((), ()))
COLS_BY_COLS = (((0,), (0,)), ((), ()))


def mxu(a, b, dims):
    return lax.dot_general(a, b, dims, preferred_element_type=jnp.float32)


def two(x):
    high = x.astype(jnp.bfloat16)
    return high, (x - high.astype(jnp.float32)).astype(jnp.bfloat16)


def three(x):
    high = x.astype(jnp.bfloat16)
    rest = x - high.astype(jnp.float32)
    middle = rest.astype(jnp.bfloat16)
    return high, middle, (rest - middle.astype(jnp.float32)).astype(jnp.bfloat16)


def product(a, b, dims):
    return mxu(a[0], b[0], dims) + (mxu(a[0], b[1], dims) + mxu(a[1], b[0], dims))


def row_gram(x):
    high, middle, low = three(x)
    side = mxu(high, middle, ROWS_BY_ROWS) + mxu(high, low, ROWS_BY_ROWS)
    return (
        mxu(high, high, ROWS_BY_ROWS) + (side + side.T) + mxu(middle, middle, ROWS_BY_ROWS)
    )


def thin_product(left, right):
    a, b, c = three(left)
    d, e, f = three(right)
    return mxu(
        jnp.concatenate([a, a, b, b, a, c], axis=0),
        jnp.concatenate([d, e, d, e, f, d], axis=0),
        COLS_BY_COLS,
    )


def eliminate_slab(work, first, size):
    tiles = STEP // 8
    lane0 = first // LANES * LANES
    rows = pl.ds(first, STEP)
    left_end = size + min(size, (first + STEP + LANES - 1) // LANES * LANES)
    lanes = list(range(lane0, size, LANES)) + list(range(size, left_end, LANES))
    diag = work[rows, pl.ds(lane0, LANES)]
    panel = [[work[pl.ds(first + 8 * t, 8), pl.ds(l, LANES)] for l in lanes] for t in range(tiles)]
    column = [
        [
            jnp.broadcast_to(
                diag[8 * t : 8 * t + 8, first - lane0 + k : first - lane0 + k + 1], (8, LANES)
            )
            for t in range(tiles)
        ]
        for k in range(STEP)
    ]
    sublane = lax.broadcasted_iota(jnp.int32, (8, LANES), 0)
    pivots = [jnp.ones((8, LANES), jnp.float32) for t in range(tiles)]

    def spread(value, row):
        return jnp.broadcast_to(value[row : row + 1, :], (8, LANES))

    for j in range(STEP):
        t0, r = divmod(j, 8)
        pivot = spread(column[j][t0], r)
        pivots[t0] = jnp.where(sublane == r, pivot, pivots[t0])
        if j == STEP - 1:
            break
        inverse = 1.0 / pivot
        pivot_row = [spread(v, r) for v in panel[t0]]
        heads = {k: spread(column[k][t0], r) for k in range(j + 1, STEP)}
        for t in range(t0, tiles):
            if t == t0 and r == 7:
                continue
            factor = column[j][t] * inverse
            if t == t0:
                factor = jnp.where(sublane > r, factor, 0.0)
            panel[t] = [v - factor * p for v, p in zip(panel[t], pivot_row)]
            for k in range(j + 1, STEP):
                column[k][t] = column[k][t] - factor * heads[k]
    roots = [lax.rsqrt(p) for p in pivots]
    panel = [[v * roots[t] for v in panel[t]] for t in range(tiles)]
    slab = jnp.concatenate([jnp.concatenate(p, axis=1) for p in panel], axis=0)
    for i, l in enumerate(lanes):
        work[rows, pl.ds(l, LANES)] = slab[:, i * LANES : (i + 1) * LANES]
    below = first + STEP
    if below < size:
        start = below // LANES * LANES
        skip = start - lane0
        update = thin_product(slab[:, skip : size - lane0], slab[:, skip:])
        rest = pl.ds(below, size - below)
        for i, l in enumerate(lanes[skip // LANES :]):
            work[rest, pl.ds(l, LANES)] = (
                work[rest, pl.ds(l, LANES)] - update[below - start :, i * LANES : (i + 1) * LANES]
            )


def inverse_factor(work, square, size):
    row = lax.broadcasted_iota(jnp.int32, (size, size), 0)
    col = lax.broadcasted_iota(jnp.int32, (size, size), 1)
    work[:, :size] = square
    work[:, size:] = (row == col).astype(jnp.float32)
    for first in range(0, size, STEP):
        eliminate_slab(work, first, size)
    return work[:, size:]


def chain_kernel(
    info, kept_a, sent_a, kept_b, sent_b, start, left, right, out_left, out_right,
    high, low, current, image, work, scale, rows_in, rows_out, in_sems, out_sems,
):
    rows = left.shape[0]
    tile = rows // SLOTS
    rank = start.shape[1]

    def fetch(side, slot):
        at = pl.ds(slot * tile, tile)
        source = (left, right)[side]
        return pltpu.make_async_copy(source.at[at, :], rows_in.at[side, at, :], in_sems.at[side, slot])

    def store(side, slot):
        at = pl.ds(slot * tile, tile)
        target = (out_left, out_right)[side]
        return pltpu.make_async_copy(rows_out.at[side, at, :], target.at[at, :], out_sems.at[side, slot])

    for side in range(2):
        for slot in range(SLOTS):
            fetch(side, slot).start()

    half = kept_a.shape[0]
    mine = info[1]
    for part, (kept, sent) in enumerate(((kept_a, sent_a), (kept_b, sent_b))):
        for ref, place in ((kept, mine), (sent, 1 - mine)):
            at = pl.ds(pl.multiple_of((2 * part + place) * half, half), half)
            high[at, :], low[at, :] = two(ref[...])
    current[0] = start[...].T

    def turn(step, carry):
        now = step % 2
        product_t = product(two(current[now]), (high[...], low[...]), ROWS_BY_ROWS)

        @pl.when(step < POWER)
        def _():
            image[...] = product(two(product_t), (high[...], low[...]), ROWS_BY_COLS)

        @pl.when(step == POWER)
        def _():
            image[...] = product_t
            scale[0] = jnp.sqrt(jnp.sum(product_t * product_t) / rank)

        inverse = inverse_factor(work, row_gram(image[...]), rank)
        current[1 - now] = product(two(inverse), two(image[...]), ROWS_BY_COLS)
        return carry

    lax.fori_loop(0, POWER + 1, turn, 0)
    right_map = product(two(work[:, rank:]), two(current[POWER % 2]), ROWS_BY_COLS) * scale[0]
    maps = (two(current[(POWER + 1) % 2]), two(right_map))
    for side in range(2):
        for slot in range(SLOTS):
            fetch(side, slot).wait()
    for side in range(2):
        for slot in range(SLOTS):
            at = pl.ds(slot * tile, tile)
            term = product(two(rows_in[side, at, :]), maps[side], ROWS_BY_ROWS)
            rows_out[side, at, :] = jnp.where(slot < info[0], term, 0.0)
            store(side, slot).start()
    for side in range(2):
        for slot in range(SLOTS):
            store(side, slot).wait()


def chain(info, kept_a, sent_a, kept_b, sent_b, start, left, right):
    states, rank = start.shape
    rows = left.shape[0]
    whole = pl.BlockSpec(memory_space=pltpu.VMEM)
    outside = pl.BlockSpec(memory_space=pl.ANY)
    return pl.pallas_call(
        chain_kernel,
        out_shape=[jax.ShapeDtypeStruct((rows, rank), jnp.float32)] * 2,
        in_specs=[pl.BlockSpec(memory_space=pltpu.SMEM)] + [whole] * 5 + [outside] * 2,
        out_specs=[outside] * 2,
        scratch_shapes=[
            pltpu.VMEM((states, states), jnp.bfloat16),
            pltpu.VMEM((states, states), jnp.bfloat16),
            pltpu.VMEM((2, rank, states), jnp.float32),
            pltpu.VMEM((rank, states), jnp.float32),
            pltpu.VMEM((rank, 2 * rank), jnp.float32),
            pltpu.SMEM((1,), jnp.float32),
            pltpu.VMEM((2, rows, states), jnp.float32),
            pltpu.VMEM((2, rows, rank), jnp.float32),
            pltpu.SemaphoreType.DMA((2, SLOTS)),
            pltpu.SemaphoreType.DMA((2, SLOTS)),
        ],
        compiler_params=pltpu.CompilerParams(vmem_limit_bytes=56 * 2**20),
        name="chain",
    )(info, kept_a, sent_a, kept_b, sent_b, start, left, right)


def gram_kernel(info, left, right, *refs):
    outs, (left_rows, right_rows, sems) = refs[: 2 * PARTS], refs[2 * PARTS :]
    rows, states = right.shape
    chunks = SLOTS * PIECES
    tile = rows // chunks
    half = outs[0].shape[0]

    def fetch(chunk):
        at = pl.ds(chunk * tile, tile)
        return (
            pltpu.make_async_copy(left.at[at, :], left_rows.at[at, :], sems.at[0, chunk]),
            pltpu.make_async_copy(right.at[at, :], right_rows.at[at, :], sems.at[1, chunk]),
        )

    for chunk in range(chunks):
        for copy in fetch(chunk):
            copy.start()
    kept_first = info[1] == 0
    for chunk in range(chunks):
        for copy in fetch(chunk):
            copy.wait()
        at = pl.ds(chunk * tile, tile)
        head, tail = two(left_rows[at, :].T)
        heads = jnp.concatenate([head, head, tail], axis=1)
        for first in range(0, states, COLUMNS):
            cols = pl.ds(first, COLUMNS)
            high, low = two(jnp.where(chunk // PIECES < info[0], right_rows[at, cols], 0.0))
            term = mxu(heads, jnp.concatenate([high, low, high], axis=0), ROWS_BY_COLS)
            for part in range(PARTS):
                top = term[2 * part * half : (2 * part + 1) * half]
                bottom = term[(2 * part + 1) * half : (2 * part + 2) * half]
                kept = jnp.where(kept_first, top, bottom)
                sent = jnp.where(kept_first, bottom, top)
                for out, value in zip(outs[2 * part : 2 * part + 2], (kept, sent)):
                    if chunk == 0:
                        out[:, cols] = value
                    else:
                        out[:, cols] += value


def gram_parts(info, left, right):
    rows, states = left.shape
    half = states // PARTS // 2
    outside = pl.BlockSpec(memory_space=pl.ANY)
    return pl.pallas_call(
        gram_kernel,
        out_shape=[jax.ShapeDtypeStruct((half, states), jnp.float32)] * (2 * PARTS),
        in_specs=[pl.BlockSpec(memory_space=pltpu.SMEM), outside, outside],
        out_specs=[pl.BlockSpec(memory_space=pltpu.VMEM)] * (2 * PARTS),
        scratch_shapes=[
            pltpu.VMEM((rows, states), jnp.float32),
            pltpu.VMEM((rows, states), jnp.float32),
            pltpu.SemaphoreType.DMA((2, SLOTS * PIECES)),
        ],
        compiler_params=pltpu.CompilerParams(vmem_limit_bytes=56 * 2**20),
        cost_estimate=pl.CostEstimate(
            flops=6 * rows * states * states, bytes_accessed=8 * rows * states, transcendentals=0
        ),
        name="gram",
    )(info, left, right)


class Pairs:
    def __init__(self, devices, bit):
        self.bit = bit
        self.table = [(i, i ^ (1 << bit)) for i in range(devices)]

    def side(self):
        return (lax.axis_index("rows") >> self.bit) & 1

    def swap(self, block):
        return lax.ppermute(block, "rows", self.table)

    def reduce_scatter(self, block):
        half = block.shape[0] // 2
        mine = self.side()
        away = self.swap(lax.dynamic_slice_in_dim(block, (1 - mine) * half, half, 0))
        return lax.dynamic_slice_in_dim(block, mine * half, half, 0) + away

    def all_gather(self, piece):
        away = self.swap(piece)
        second = self.side() == 1
        return jnp.concatenate(
            [jnp.where(second, away, piece), jnp.where(second, piece, away)], axis=0
        )


def make_local(devices):
    bits = devices.bit_length() - 1
    core = Pairs(devices, 0)
    others = [Pairs(devices, bit) for bit in range(1, bits)]
    orders = (others, others[1:] + others[:1])

    def local(left_factor, right_factor, tile_counts, start_basis):
        side = core.side()
        info = jnp.stack([tile_counts[0], side]).astype(jnp.int32)
        terms = gram_parts(info, left_factor, right_factor)
        blocks = []
        for kept, sent, order in zip(terms[::2], terms[1::2], orders):
            block = kept + core.swap(sent)
            for pairs in order[:-1]:
                block = pairs.reduce_scatter(block)
            block = block + order[-1].swap(block)
            for pairs in reversed(order[:-1]):
                block = pairs.all_gather(block)
            blocks += [block, core.swap(block)]
        return tuple(chain(info, *blocks, start_basis, left_factor, right_factor))

    return local


def solution(mesh):
    return jax.shard_map(
        make_local(mesh.shape["rows"]),
        mesh=mesh,
        in_specs=(P("rows", None), P("rows", None), P("rows"), P()),
        out_specs=(P("rows", None), P("rows", None)),
        check_vma=False,
    )
```

```python
import functools

import jax
import jax.numpy as jnp
from jax import lax
from jax.experimental import pallas as pl
from jax.experimental.pallas import tpu as pltpu
from jax.sharding import PartitionSpec as P

SLOTS = 4
POWER = 2
STEP = 32
GROUP = 16
COLUMNS = 256
PARTS = 2
PIECES = 1
LANES = 128

ROWS_BY_ROWS = (((1,), (1,)), ((), ()))
ROWS_BY_COLS = (((1,), (0,)), ((), ()))
COLS_BY_COLS = (((0,), (0,)), ((), ()))


def mxu(a, b, dims):
    return lax.dot_general(a, b, dims, preferred_element_type=jnp.float32)


def two(x):
    high = x.astype(jnp.bfloat16)
    return high, (x - high.astype(jnp.float32)).astype(jnp.bfloat16)


def three(x):
    high = x.astype(jnp.bfloat16)
    rest = x - high.astype(jnp.float32)
    middle = rest.astype(jnp.bfloat16)
    return high, middle, (rest - middle.astype(jnp.float32)).astype(jnp.bfloat16)


def product(a, b, dims):
    return mxu(a[0], b[0], dims) + (mxu(a[0], b[1], dims) + mxu(a[1], b[0], dims))


def row_gram(x):
    high, middle, low = three(x)
    side = mxu(high, middle, ROWS_BY_ROWS) + mxu(high, low, ROWS_BY_ROWS)
    return (
        mxu(high, high, ROWS_BY_ROWS) + (side + side.T) + mxu(middle, middle, ROWS_BY_ROWS)
    )


def thin_product(left, right):
    a, b, c = three(left)
    d, e, f = three(right)
    return mxu(
        jnp.concatenate([a, a, b, b, a, c], axis=0),
        jnp.concatenate([d, e, d, e, f, d], axis=0),
        COLS_BY_COLS,
    )


def eliminate_slab(work, first, size):
    tiles = STEP // 8
    lane0 = first // LANES * LANES
    rows = pl.ds(first, STEP)
    left_end = size + min(size, (first + STEP + LANES - 1) // LANES * LANES)
    lanes = list(range(lane0, size, LANES)) + list(range(size, left_end, LANES))
    panel = [[work[pl.ds(first + 8 * t, 8), pl.ds(l, LANES)] for l in lanes] for t in range(tiles)]
    sublane = lax.broadcasted_iota(jnp.int32, (8, LANES), 0)
    pivots = [jnp.ones((8, LANES), jnp.float32) for t in range(tiles)]

    def spread(value, row):
        return jnp.broadcast_to(value[row : row + 1, :], (8, LANES))

    for j in range(0, STEP, 2):
        t0, r = divmod(j, 8)
        if j % GROUP == 0:
            column = {
                k: [
                    jnp.broadcast_to(v[0][:, first - lane0 + k : first - lane0 + k + 1], (8, LANES))
                    for v in panel
                ]
                for k in range(j, j + GROUP)
            }
        end = j // GROUP * GROUP + GROUP
        first_pivot = spread(column[j][t0], r)
        cross = spread(column[j][t0], r + 1)
        corner = spread(column[j + 1][t0], r + 1)
        ratio = cross / first_pivot
        second_pivot = corner - ratio * cross
        pivots[t0] = jnp.where(sublane == r, first_pivot, pivots[t0])
        pivots[t0] = jnp.where(sublane == r + 1, second_pivot, pivots[t0])
        inverse = 1.0 / (first_pivot * corner - cross * cross)
        pivot_rows = [(spread(v, r), spread(v, r + 1)) for v in panel[t0]]
        heads = {
            k: (spread(column[k][t0], r), spread(column[k][t0], r + 1)) for k in range(j + 2, end)
        }
        for t in range(t0, tiles):
            x, y = column[j][t], column[j + 1][t]
            one = (x * corner - y * cross) * inverse
            other = (y * first_pivot - x * cross) * inverse
            if t == t0:
                one = jnp.where(sublane > r + 1, one, jnp.where(sublane == r + 1, ratio, 0.0))
                other = jnp.where(sublane > r + 1, other, 0.0)
            panel[t] = [v - (one * p + other * q) for v, (p, q) in zip(panel[t], pivot_rows)]
            for k in range(j + 2, end):
                column[k][t] = column[k][t] - (one * heads[k][0] + other * heads[k][1])
    roots = [lax.rsqrt(p) for p in pivots]
    panel = [[v * roots[t] for v in panel[t]] for t in range(tiles)]
    slab = jnp.concatenate([jnp.concatenate(p, axis=1) for p in panel], axis=0)
    for i, l in enumerate(lanes):
        work[rows, pl.ds(l, LANES)] = slab[:, i * LANES : (i + 1) * LANES]
    below = first + STEP
    if below < size:
        start = below // LANES * LANES
        skip = start - lane0
        update = thin_product(slab[:, skip : size - lane0], slab[:, skip:])
        rest = pl.ds(below, size - below)
        for i, l in enumerate(lanes[skip // LANES :]):
            work[rest, pl.ds(l, LANES)] = (
                work[rest, pl.ds(l, LANES)] - update[below - start :, i * LANES : (i + 1) * LANES]
            )


def inverse_factor(work, square, size):
    row = lax.broadcasted_iota(jnp.int32, (size, size), 0)
    col = lax.broadcasted_iota(jnp.int32, (size, size), 1)
    work[:, :size] = square
    work[:, size:] = (row == col).astype(jnp.float32)
    for first in range(0, size, STEP):
        eliminate_slab(work, first, size)
    return work[:, size:]


def chain_kernel(
    info, kept_a, sent_a, kept_b, sent_b, start, left, right, out_left, out_right,
    high, low, current, image, unit, work, row_scale, scale, rows_in, rows_out, in_sems, out_sems,
):
    rows = left.shape[0]
    tile = rows // SLOTS
    rank = start.shape[1]

    def fetch(side, slot):
        at = pl.ds(slot * tile, tile)
        source = (left, right)[side]
        return pltpu.make_async_copy(source.at[at, :], rows_in.at[side, at, :], in_sems.at[side, slot])

    def store(side, slot):
        at = pl.ds(slot * tile, tile)
        target = (out_left, out_right)[side]
        return pltpu.make_async_copy(rows_out.at[side, at, :], target.at[at, :], out_sems.at[side, slot])

    for side in range(2):
        for slot in range(SLOTS):
            fetch(side, slot).start()

    half = kept_a.shape[0]
    mine = info[1]
    for part, (kept, sent) in enumerate(((kept_a, sent_a), (kept_b, sent_b))):
        for ref, place in ((kept, mine), (sent, 1 - mine)):
            at = pl.ds(pl.multiple_of((2 * part + place) * half, half), half)
            high[at, :], low[at, :] = two(ref[...])
    current[0] = start[...].T

    def turn(step, carry):
        now = step % 2
        product_t = product(two(current[now]), (high[...], low[...]), ROWS_BY_ROWS)

        @pl.when(step < POWER)
        def _():
            image[...] = product(two(product_t), (high[...], low[...]), ROWS_BY_COLS)

        @pl.when(step == POWER)
        def _():
            image[...] = product_t

        norms = jnp.sum(image[...] * image[...], axis=1, keepdims=True)
        scale[0] = jnp.sqrt(jnp.sum(norms) / rank)
        roots = lax.rsqrt(norms)
        unit[...] = image[...] * roots
        row_scale[...] = roots
        inverse = inverse_factor(work, row_gram(unit[...]), rank)
        current[1 - now] = product(two(inverse), two(unit[...]), ROWS_BY_COLS)
        return carry

    lax.fori_loop(0, POWER + 1, turn, 0)
    scaled = current[POWER % 2] * (row_scale[...] * scale[0])
    right_map = product(two(work[:, rank:]), two(scaled), ROWS_BY_COLS)
    maps = (two(current[(POWER + 1) % 2]), two(right_map))
    for side in range(2):
        for slot in range(SLOTS):
            fetch(side, slot).wait()
    for side in range(2):
        for slot in range(SLOTS):
            at = pl.ds(slot * tile, tile)
            term = product(two(rows_in[side, at, :]), maps[side], ROWS_BY_ROWS)
            rows_out[side, at, :] = jnp.where(slot < info[0], term, 0.0)
            store(side, slot).start()
    for side in range(2):
        for slot in range(SLOTS):
            store(side, slot).wait()


def chain(info, kept_a, sent_a, kept_b, sent_b, start, left, right):
    states, rank = start.shape
    rows = left.shape[0]
    whole = pl.BlockSpec(memory_space=pltpu.VMEM)
    outside = pl.BlockSpec(memory_space=pl.ANY)
    return pl.pallas_call(
        chain_kernel,
        out_shape=[jax.ShapeDtypeStruct((rows, rank), jnp.float32)] * 2,
        in_specs=[pl.BlockSpec(memory_space=pltpu.SMEM)] + [whole] * 5 + [outside] * 2,
        out_specs=[outside] * 2,
        scratch_shapes=[
            pltpu.VMEM((states, states), jnp.bfloat16),
            pltpu.VMEM((states, states), jnp.bfloat16),
            pltpu.VMEM((2, rank, states), jnp.float32),
            pltpu.VMEM((rank, states), jnp.float32),
            pltpu.VMEM((rank, states), jnp.float32),
            pltpu.VMEM((rank, 2 * rank), jnp.float32),
            pltpu.VMEM((rank, 1), jnp.float32),
            pltpu.SMEM((1,), jnp.float32),
            pltpu.VMEM((2, rows, states), jnp.float32),
            pltpu.VMEM((2, rows, rank), jnp.float32),
            pltpu.SemaphoreType.DMA((2, SLOTS)),
            pltpu.SemaphoreType.DMA((2, SLOTS)),
        ],
        compiler_params=pltpu.CompilerParams(vmem_limit_bytes=56 * 2**20),
        name="chain",
    )(info, kept_a, sent_a, kept_b, sent_b, start, left, right)


def gram_kernel(info, left, right, *refs):
    outs, (left_rows, right_rows, sems) = refs[: 2 * PARTS], refs[2 * PARTS :]
    rows, states = right.shape
    chunks = SLOTS * PIECES
    tile = rows // chunks
    half = outs[0].shape[0]

    def fetch(chunk):
        at = pl.ds(chunk * tile, tile)
        return (
            pltpu.make_async_copy(left.at[at, :], left_rows.at[at, :], sems.at[0, chunk]),
            pltpu.make_async_copy(right.at[at, :], right_rows.at[at, :], sems.at[1, chunk]),
        )

    for chunk in range(chunks):
        for copy in fetch(chunk):
            copy.start()
    kept_first = info[1] == 0
    for chunk in range(chunks):
        for copy in fetch(chunk):
            copy.wait()
        at = pl.ds(chunk * tile, tile)
        head, tail = two(left_rows[at, :].T)
        heads = jnp.concatenate([head, head, tail], axis=1)
        for first in range(0, states, COLUMNS):
            cols = pl.ds(first, COLUMNS)
            high, low = two(jnp.where(chunk // PIECES < info[0], right_rows[at, cols], 0.0))
            term = mxu(heads, jnp.concatenate([high, low, high], axis=0), ROWS_BY_COLS)
            for part in range(PARTS):
                top = term[2 * part * half : (2 * part + 1) * half]
                bottom = term[(2 * part + 1) * half : (2 * part + 2) * half]
                kept = jnp.where(kept_first, top, bottom)
                sent = jnp.where(kept_first, bottom, top)
                for out, value in zip(outs[2 * part : 2 * part + 2], (kept, sent)):
                    if chunk == 0:
                        out[:, cols] = value
                    else:
                        out[:, cols] += value


def gram_parts(info, left, right):
    rows, states = left.shape
    half = states // PARTS // 2
    outside = pl.BlockSpec(memory_space=pl.ANY)
    return pl.pallas_call(
        gram_kernel,
        out_shape=[jax.ShapeDtypeStruct((half, states), jnp.float32)] * (2 * PARTS),
        in_specs=[pl.BlockSpec(memory_space=pltpu.SMEM), outside, outside],
        out_specs=[pl.BlockSpec(memory_space=pltpu.VMEM)] * (2 * PARTS),
        scratch_shapes=[
            pltpu.VMEM((rows, states), jnp.float32),
            pltpu.VMEM((rows, states), jnp.float32),
            pltpu.SemaphoreType.DMA((2, SLOTS * PIECES)),
        ],
        compiler_params=pltpu.CompilerParams(vmem_limit_bytes=56 * 2**20),
        cost_estimate=pl.CostEstimate(
            flops=6 * rows * states * states, bytes_accessed=8 * rows * states, transcendentals=0
        ),
        name="gram",
    )(info, left, right)


class Pairs:
    def __init__(self, devices, bit):
        self.bit = bit
        self.table = [(i, i ^ (1 << bit)) for i in range(devices)]

    def side(self):
        return (lax.axis_index("rows") >> self.bit) & 1

    def swap(self, block):
        return lax.ppermute(block, "rows", self.table)

    def reduce_scatter(self, block):
        half = block.shape[0] // 2
        mine = self.side()
        away = self.swap(lax.dynamic_slice_in_dim(block, (1 - mine) * half, half, 0))
        return lax.dynamic_slice_in_dim(block, mine * half, half, 0) + away

    def all_gather(self, piece):
        away = self.swap(piece)
        second = self.side() == 1
        return jnp.concatenate(
            [jnp.where(second, away, piece), jnp.where(second, piece, away)], axis=0
        )


def make_local(devices):
    bits = devices.bit_length() - 1
    core = Pairs(devices, 0)
    others = [Pairs(devices, bit) for bit in range(1, bits)]
    orders = (others, others[1:] + others[:1])

    def local(left_factor, right_factor, tile_counts, start_basis):
        side = core.side()
        info = jnp.stack([tile_counts[0], side]).astype(jnp.int32)
        terms = gram_parts(info, left_factor, right_factor)
        blocks = []
        for kept, sent, order in zip(terms[::2], terms[1::2], orders):
            block = kept + core.swap(sent)
            for pairs in order[:-1]:
                block = pairs.reduce_scatter(block)
            block = block + order[-1].swap(block)
            for pairs in reversed(order[:-1]):
                block = pairs.all_gather(block)
            blocks += [block, core.swap(block)]
        return tuple(chain(info, *blocks, start_basis, left_factor, right_factor))

    return local


def solution(mesh):
    return jax.shard_map(
        make_local(mesh.shape["rows"]),
        mesh=mesh,
        in_specs=(P("rows", None), P("rows", None), P("rows"), P()),
        out_specs=(P("rows", None), P("rows", None)),
        check_vma=False,
    )
```
